256 devices in a mesh: row: 16 (over x_hi, z), col: 16 (over x_lo, y, core).
Axes of the slice: x: 4 (x_hi: 2, x_lo: 2; x = x_hi * 2 + x_lo), y: 4, z: 8, core: 2. Of those that a mesh axis runs over, the one named last changes fastest.
Arguments:
- southeast_edges: bfloat16 [16, 16, 2, 2, 2, 96, 768], P('row', 'col'), may hold values from -6 to 6
- northwest_edges: bfloat16 [16, 16, 2, 2, 2, 96, 768], P('row', 'col'), may hold values from -6 to 6
- southeast_corners: bfloat16 [16, 16, 2, 2, 96, 128], P('row', 'col'), may hold values from -6 to 6
- northwest_corners: bfloat16 [16, 16, 2, 2, 96, 128], P('row', 'col'), may hold values from -6 to 6
- operators: bfloat16 [16, 16, 2, 2, 768, 768], P('row', 'col'), may hold values from -0.109375 to 0.109375
- sources: bfloat16 [16, 16, 2, 2, 96, 768], P('row', 'col'), may hold values from -3 to 3
- roster: int32 [2, 3, 2], replicated, may hold values from 0 to 1, as said below
Outputs:
- southeast_out: bfloat16 [16, 16, 2, 2, 2, 96, 768], P('row', 'col')
- northwest_out: bfloat16 [16, 16, 2, 2, 2, 96, 768], P('row', 'col')
- southeast_corner_out: bfloat16 [16, 16, 2, 2, 96, 128], P('row', 'col')
- northwest_corner_out: bfloat16 [16, 16, 2, 2, 96, 128], P('row', 'col')
The draws below stay inside these ranges and needn't reach their ends.
Inputs may be any that keep to these rules, and one draw needn't show every extreme that they name: roster[d, k, b] is the class, modulo 2, of the antidiagonals on which batch b of direction d stands at tick k. It rises by one modulo 2 from each tick to the next, and at every tick the 2 batches of one direction take all classes, each once.
All inputs are finite; a program needn't handle non-finite values.
Results may differ from the reference program's by a relative error of at most 0.0051.
Values may be sent and summed in bfloat16 or wider, within the bound.
A program may use at most 64 MiB of HBM per device.

```python
import jax
import jax.numpy as jnp
from jax import lax

EDGE = 768
CORNER = 128
SHOTS = 96
BATCHES = 2
TICKS = 3
NR = 16
NC = 16


def draw_roster(key, part):
    ticks_column = jnp.arange(TICKS, dtype=jnp.int32)[:, None]
    planes = []
    for direction in range(2):
        subkey = jax.random.fold_in(key, 17 + direction)
        start = jax.random.randint(jax.random.fold_in(subkey, 1), (), 0, BATCHES).astype(jnp.int32)
        order = jax.random.permutation(jax.random.fold_in(subkey, 2), BATCHES).astype(jnp.int32)
        planes.append(jnp.mod(order[None, :] + start + ticks_column, BATCHES).astype(jnp.int32))
    return jnp.stack(planes).astype(jnp.int32)


def block_levels(own_key, extent, cuts, smallest, top_value):
    def one(position, parts):
        steps = jax.random.uniform(jax.random.fold_in(jax.random.fold_in(own_key, 6), position), (parts,), jnp.float32, smallest / len(cuts), top_value / len(cuts))
        return jnp.repeat(jnp.exp(steps), extent[position] // parts).reshape((-1,) + (1,) * (len(extent) - position - 1))

    factor_of = one(*cuts[0])
    for cut in cuts[1:]:
        factor_of = factor_of * one(*cut)
    return factor_of


def bell_draw(own_key, shape, width, most, split=(), kind=jnp.bfloat16):
    array = width * jax.random.normal(own_key, shape, jnp.float32)
    if split:
        array = array * block_levels(own_key, shape, split, -0.22, 0.18)
    return jnp.clip(array, -most, most).astype(kind)


def setup_inputs(seed: int = 0) -> dict:
    keys = jax.random.split(jax.random.key(seed), 8)
    southeast_edges = bell_draw(keys[0], (NR, NC, 2, BATCHES, 2, SHOTS, EDGE), 1.0, 6.0, ((0, 16), (1, 16)))
    northwest_edges = bell_draw(keys[1], (NR, NC, 2, BATCHES, 2, SHOTS, EDGE), 1.0, 6.0, ((0, 16), (1, 16)))
    southeast_corners = bell_draw(keys[2], (NR, NC, BATCHES, 2, SHOTS, CORNER), 1.0, 6.0, ((0, 16), (1, 16)))
    northwest_corners = bell_draw(keys[3], (NR, NC, BATCHES, 2, SHOTS, CORNER), 1.0, 6.0, ((0, 16), (1, 16)))
    operators = bell_draw(keys[4], (NR, NC, 2, 2, EDGE, EDGE), (4 * EDGE) ** -0.5, 0.109375, ((0, 16), (1, 16)))
    sources = bell_draw(keys[5], (NR, NC, BATCHES, 2, SHOTS, EDGE), 0.5, 3.0, ((0, 16), (1, 16)))
    roster = draw_roster(jax.random.fold_in(keys[7], 71), 0)
    return dict(southeast_edges=southeast_edges, northwest_edges=northwest_edges, southeast_corners=southeast_corners, northwest_corners=northwest_corners, operators=operators, sources=sources, roster=roster)


def trace_update(first_in, second_in, corner_in, cell_operators, source, flipped):
    shot_count = first_in.shape[1]
    edge_width = first_in.shape[2]
    corner_width = corner_in.shape[-1]
    stacked = jnp.stack([first_in, second_in]).reshape(4 * shot_count, edge_width).astype(jnp.float32)
    form = "qe,mpfe->mpqf" if flipped else "qe,mpef->mpqf"
    products = jnp.einsum(form, stacked, cell_operators.astype(jnp.float32), precision=lax.Precision.HIGHEST)
    products = products.reshape(2, 2, 2, 2, shot_count, edge_width)

    def complex_product(source_index, operator_index):
        real_part = products[operator_index, 0, source_index, 0] - products[operator_index, 1, source_index, 1]
        imag_part = products[operator_index, 1, source_index, 0] + products[operator_index, 0, source_index, 1]
        return jnp.stack([real_part, imag_part])

    source_value = source.astype(jnp.float32)
    corner_value = corner_in.astype(jnp.float32)
    first_out = complex_product(0, 0) + complex_product(1, 1) + source_value
    second_out = complex_product(0, 1) + complex_product(1, 0) + source_value
    if flipped:
        first_out = first_out.at[:, :, edge_width - corner_width:].add(corner_value)
        second_out = second_out.at[:, :, edge_width - corner_width:].add(corner_value)
        corner_out = 0.5 * (first_out[:, :, :corner_width] + second_out[:, :, :corner_width])
    else:
        first_out = first_out.at[:, :, :corner_width].add(corner_value)
        second_out = second_out.at[:, :, :corner_width].add(corner_value)
        corner_out = 0.5 * (first_out[:, :, edge_width - corner_width:] + second_out[:, :, edge_width - corner_width:])
    return first_out.astype(jnp.bfloat16), second_out.astype(jnp.bfloat16), corner_out.astype(jnp.bfloat16)


def sweep_tick(states, corner_states, operators, sources, plan, flipped):
    cell_numbers = jnp.arange(NR * NC, dtype=jnp.int32)
    row_numbers = (cell_numbers // NC).astype(jnp.int32)
    col_numbers = (cell_numbers % NC).astype(jnp.int32)
    offset = 1 if flipped else -1

    def one_cell(packed):
        row_index, col_index = packed
        if flipped:
            klass = jnp.mod((NR - 1 - row_index) + (NC - 1 - col_index), BATCHES)
        else:
            klass = jnp.mod(row_index + col_index, BATCHES)
        batch_index = jnp.argmax((plan == klass).astype(jnp.int32)).astype(jnp.int32)
        near_row = jnp.mod(row_index + offset, NR).astype(jnp.int32)
        near_col = jnp.mod(col_index + offset, NC).astype(jnp.int32)
        first_in = states[near_row, col_index, 0, batch_index]
        second_in = states[row_index, near_col, 1, batch_index]
        corner_in = corner_states[near_row, near_col, batch_index]
        first_out, second_out, corner_out = trace_update(first_in, second_in, corner_in,
                                                         operators[row_index, col_index],
                                                         sources[row_index, col_index, batch_index], flipped)
        return first_out, second_out, corner_out, batch_index

    firsts, seconds, corner_outs, batch_list = lax.map(one_cell, (row_numbers, col_numbers))
    renewed = states.at[row_numbers, col_numbers, 0, batch_list].set(firsts)
    renewed = renewed.at[row_numbers, col_numbers, 1, batch_list].set(seconds)
    renewed_corners = corner_states.at[row_numbers, col_numbers, batch_list].set(corner_outs)
    return renewed, renewed_corners


def reference(southeast_edges, northwest_edges, southeast_corners, northwest_corners, operators, sources, roster):
    down_states, up_states = southeast_edges, northwest_edges
    down_corners, up_corners = southeast_corners, northwest_corners
    for tick_index in range(TICKS):
        down_states, down_corners = sweep_tick(down_states, down_corners, operators, sources,
                                               roster[0, tick_index], False)
        up_states, up_corners = sweep_tick(up_states, up_corners, operators, sources,
                                           roster[1, tick_index], True)
    return down_states, up_states, down_corners, up_corners
```

```python
import jax
import jax.numpy as jnp
from jax import lax
from jax.experimental import pallas as pl
from jax.experimental.pallas import tpu as pltpu
from jax.sharding import PartitionSpec as P

MESH = pl.DeviceIdType.MESH
TICKS = 3
CHUNKS = 2


def sweep_kernel(
    sizes,
    roster,
    se_edges,
    nw_edges,
    se_corners,
    nw_corners,
    operators,
    sources,
    se_out,
    nw_out,
    se_corner_out,
    nw_corner_out,
    held_se,
    held_nw,
    weights,
    flipped,
    source,
    sent,
    got,
    start_se,
    start_nw,
    corner_got,
    corner_now,
    corner_new,
    plan,
    load_sem,
    send_sem,
    recv_sem,
    corner_send_sem,
    corner_recv_sem,
):
    row_count, col_count, shots, width, corner = sizes
    part = shots // CHUNKS
    row = lax.axis_index("row")
    col = lax.axis_index("col")
    down = lax.rem(row + 1, row_count)
    up = lax.rem(row + row_count - 1, row_count)
    right = lax.rem(col + 1, col_count)
    left = lax.rem(col + col_count - 1, col_count)
    ahead = (
        ((down, col), (row, right), (down, right)),
        ((up, col), (row, left), (up, left)),
    )

    loads = [
        pltpu.make_async_copy(se_edges, held_se, load_sem.at[0]),
        pltpu.make_async_copy(nw_edges, held_nw, load_sem.at[1]),
        pltpu.make_async_copy(operators, weights, load_sem.at[2]),
        pltpu.make_async_copy(sources, source, load_sem.at[3]),
        pltpu.make_async_copy(roster, plan, load_sem.at[4]),
    ]
    for load in loads:
        load.start()

    barrier = pltpu.get_barrier_semaphore()
    for direction in ahead:
        for place in direction:
            pl.semaphore_signal(barrier, inc=1, device_id=place, device_id_type=MESH)

    loads[4].wait()
    klass = lax.rem(row + col, 2)
    first = [jnp.where(plan[d, 0, 0] == klass, 0, 1) for d in range(2)]

    def edge_copy(k, d, slot, chunk):
        return pltpu.make_async_remote_copy(
            src_ref=sent.at[k, d, slot, chunk],
            dst_ref=got.at[k, d, slot, chunk],
            send_sem=send_sem.at[k, d, slot, chunk],
            recv_sem=recv_sem.at[k, d, slot, chunk],
            device_id=ahead[d][slot],
            device_id_type=MESH,
        )

    def corner_start_copy(d):
        return pltpu.make_async_remote_copy(
            src_ref=(se_corners, nw_corners)[d],
            dst_ref=(start_se, start_nw)[d],
            send_sem=corner_send_sem.at[0, d],
            recv_sem=corner_recv_sem.at[0, d],
            device_id=ahead[d][2],
            device_id_type=MESH,
        )

    def corner_copy(d):
        return pltpu.make_async_remote_copy(
            src_ref=corner_new.at[d],
            dst_ref=corner_got.at[d],
            send_sem=corner_send_sem.at[1, d],
            recv_sem=corner_recv_sem.at[1, d],
            device_id=ahead[d][2],
            device_id_type=MESH,
        )

    for d in range(2):
        loads[d].wait()
        for chunk in range(CHUNKS):
            for slot in range(2):
                sent[0, d, slot, chunk] = (held_se, held_nw)[d][slot, 1 - first[d], :, chunk * part : (chunk + 1) * part, :]
    pl.semaphore_wait(barrier, 6)
    for chunk in range(CHUNKS):
        for d in range(2):
            for slot in range(2):
                edge_copy(0, d, slot, chunk).start()
    for d in range(2):
        corner_start_copy(d).start()

    loads[2].wait()
    for m in range(4):
        flipped[m] = weights[m].T
    loads[3].wait()
    def update(k, d, chunk):
        rows = slice(chunk * part, (chunk + 1) * part)
        batch = lax.rem(first[d] + k, 2)
        for slot in range(2):
            edge_copy(k, d, slot, chunk).wait_recv()
        a_re, a_im = got[k, d, 0, chunk, 0], got[k, d, 0, chunk, 1]
        b_re, b_im = got[k, d, 1, chunk, 0], got[k, d, 1, chunk, 1]
        table = (weights, flipped)[d]
        stacks = (
            (a_re, a_im, b_re, b_im),
            (-a_im, a_re, -b_im, b_re),
            (b_re, b_im, a_re, a_im),
            (-b_im, b_re, -a_im, a_re),
        )
        total = None
        for m, stack in enumerate(stacks):
            term = jnp.dot(jnp.concatenate(stack, 0), table[m], preferred_element_type=jnp.float32)
            total = term if total is None else total + term
        total = total.reshape(2, 2, part, width)
        near, far = slice(0, corner), slice(width - corner, width)
        if d == 1:
            near, far = far, near
        for plane in range(2):
            extra = source[batch, plane, rows, :].astype(jnp.float32)
            cornered = corner_now[d, plane, rows, :].astype(jnp.float32)
            both = []
            for slot in range(2):
                value = total[slot, plane] + extra
                if d == 0:
                    value = jnp.concatenate([value[:, near] + cornered, value[:, corner:]], 1)
                else:
                    value = jnp.concatenate([value[:, : width - corner], value[:, near] + cornered], 1)
                both.append(value[:, far])
                value = value.astype(jnp.bfloat16)

                @pl.when(k < 2)
                def _():
                    sent[k + 1, d, slot, chunk, plane] = value

                @pl.when(k >= 1)
                def _():
                    (se_out, nw_out)[d][2 - k, slot, chunk, plane] = value

            value = (0.5 * (both[0] + both[1])).astype(jnp.bfloat16)

            @pl.when(k == 0)
            def _():
                corner_new[d, plane, rows, :] = value

            @pl.when(k >= 1)
            def _():
                (se_corner_out, nw_corner_out)[d][2 - k, plane, rows, :] = value


    def tick(k, carry):
        for d in range(2):

            @pl.when(k == 0)
            def _():
                corner_start_copy(d).wait_recv()

            @pl.when(k < 2)
            def _():
                corner_now[d] = (start_se, start_nw)[d][lax.rem(first[d] + k, 2)]

            @pl.when(k == 2)
            def _():
                corner_copy(d).wait_recv()
                corner_now[d] = corner_got[d]

        for chunk in range(CHUNKS):
            for d in range(2):
                update(k, d, chunk)

                @pl.when(k < 2)
                def _():
                    for slot in range(2):
                        edge_copy(k + 1, d, slot, chunk).start()

                if chunk == CHUNKS - 1:

                    @pl.when(k == 0)
                    def _():
                        corner_copy(d).start()

        return carry

    lax.fori_loop(0, TICKS, tick, 0)

    for d in range(2):
        corner_start_copy(d).wait_send()
        corner_copy(d).wait_send()
        for slot in range(2):
            for chunk in range(CHUNKS):
                for k in range(TICKS):
                    edge_copy(k, d, slot, chunk).wait_send()


def place_kernel(roster, se, nw, se_corner, nw_corner, se_out, nw_out, se_corner_out, nw_corner_out, plan, sem, plan_sem):
    load = pltpu.make_async_copy(roster, plan, plan_sem)
    load.start()
    load.wait()
    klass = lax.rem(lax.axis_index("row") + lax.axis_index("col"), 2)
    part = se.shape[4]
    copies = []
    for d in range(2):
        first = jnp.where(plan[d, 0, 0] == klass, 0, 1)
        for late in range(2):
            batch = first if late == 0 else 1 - first
            copies.append(((se_corner, nw_corner)[d].at[late], (se_corner_out, nw_corner_out)[d].at[batch]))
            for slot in range(2):
                for chunk in range(CHUNKS):
                    copies.append(
                        (
                            (se, nw)[d].at[late, slot, chunk],
                            (se_out, nw_out)[d].at[slot, batch, :, pl.ds(chunk * part, part), :],
                        )
                    )
    copies = [pltpu.make_async_copy(a, b, sem.at[i]) for i, (a, b) in enumerate(copies)]
    for copy in copies:
        copy.start()
    for copy in copies:
        copy.wait()


def shards(
    southeast_edges,
    northwest_edges,
    southeast_corners,
    northwest_corners,
    operators,
    sources,
    roster,
):
    row_count, col_count = lax.axis_size("row"), lax.axis_size("col")
    shots, width = sources.shape[-2:]
    corner = southeast_corners.shape[-1]
    part = shots // CHUNKS
    sizes = (row_count, col_count, shots, width, corner)
    anywhere = pl.BlockSpec(memory_space=pltpu.HBM)
    inside = pl.BlockSpec(memory_space=pltpu.VMEM)
    part_shape = jax.ShapeDtypeStruct((2, 2, CHUNKS, 2, part, width), jnp.bfloat16)
    edge_shape = jax.ShapeDtypeStruct((2, 2, 2, shots, width), jnp.bfloat16)
    corner_shape = jax.ShapeDtypeStruct((2, 2, shots, corner), jnp.bfloat16)
    bf16 = jnp.bfloat16
    plan = jnp.swapaxes(roster, 1, 2)
    results = pl.pallas_call(
        lambda *refs: sweep_kernel(sizes, *refs),
        out_shape=tuple(
            pltpu.VMEM(shape.shape, shape.dtype)
            for shape in (part_shape, part_shape, corner_shape, corner_shape)
        ),
        in_specs=[anywhere] * 7,
        out_specs=(inside,) * 4,
        scratch_shapes=[
            pltpu.VMEM((2, 2, 2, shots, width), bf16),
            pltpu.VMEM((2, 2, 2, shots, width), bf16),
            pltpu.VMEM((4, width, width), bf16),
            pltpu.VMEM((4, width, width), bf16),
            pltpu.VMEM((2, 2, shots, width), bf16),
            pltpu.VMEM((TICKS, 2, 2, CHUNKS, 2, part, width), bf16),
            pltpu.VMEM((TICKS, 2, 2, CHUNKS, 2, part, width), bf16),
            pltpu.VMEM((2, 2, shots, corner), bf16),
            pltpu.VMEM((2, 2, shots, corner), bf16),
            pltpu.VMEM((2, 2, shots, corner), bf16),
            pltpu.VMEM((2, 2, shots, corner), bf16),
            pltpu.VMEM((2, 2, shots, corner), bf16),
            pltpu.SMEM((2, 2, TICKS), jnp.int32),
            pltpu.SemaphoreType.DMA((5,)),
            pltpu.SemaphoreType.DMA((TICKS, 2, 2, CHUNKS)),
            pltpu.SemaphoreType.DMA((TICKS, 2, 2, CHUNKS)),
            pltpu.SemaphoreType.DMA((2, 2)),
            pltpu.SemaphoreType.DMA((2, 2)),
        ],
        compiler_params=pltpu.CompilerParams(
            collective_id=0, has_side_effects=True, vmem_limit_bytes=40 << 20
        ),
        name="sweep",
    )(
        *(
            pltpu.with_memory_space_constraint(array, pltpu.HBM)
            for array in (
                plan,
                southeast_edges[0, 0],
                northwest_edges[0, 0],
                southeast_corners[0, 0],
                northwest_corners[0, 0],
                operators[0, 0].reshape(4, width, width),
                sources[0, 0],
            )
        )
    )
    outs = pl.pallas_call(
        place_kernel,
        out_shape=(edge_shape, edge_shape, corner_shape, corner_shape),
        in_specs=[anywhere] + [inside] * 4,
        out_specs=(anywhere,) * 4,
        scratch_shapes=[
            pltpu.SMEM((2, 2, TICKS), jnp.int32),
            pltpu.SemaphoreType.DMA((4 + 8 * CHUNKS,)),
            pltpu.SemaphoreType.DMA,
        ],
        compiler_params=pltpu.CompilerParams(vmem_limit_bytes=8 << 20),
        name="place",
    )(plan, *results)
    return tuple(out[None, None] for out in outs)


def solution(mesh):
    edges = P("row", "col", None, None, None, None, None)
    corners = P("row", "col", None, None, None, None)
    return jax.shard_map(
        shards,
        mesh=mesh,
        in_specs=(edges, edges, corners, corners, corners, corners, P()),
        out_specs=(edges, edges, corners, corners),
        check_vma=False,
    )
```
